256 devices in a mesh: samp: 64 (over y, z, core), var: 4 (over x).
Axes of the slice: x: 4, y: 4, z: 8, core: 2. Of those that a mesh axis runs over, the one named last changes fastest.
Arguments:
- phenotype: float32 [65536], replicated, may hold values from -6 to 6
- perm_index: int32 [64, 65536], P(None, 'samp'), may hold values from 0 to 65535, each once within a row
- genotypes: bfloat16 [65536, 8192], P('samp', 'var'), may hold values from 0 to 2
Outputs:
- statistics: float32 [64, 8192], P('samp', 'var')
- largest: float32 [64], P('samp')
The draws below stay inside these ranges and needn't reach their ends.
Inputs may be any that keep to these rules, and one draw needn't show every extreme that they name: Each row of perm_index is a permutation of 0 to 65535.
All inputs are finite; a program needn't handle non-finite values.
Results may differ from the reference program's by a relative error of at most 0.003.
Values sent between devices are 32-bit elements; how exact they have to be, the bound alone decides.
A program may use at most 64 MiB of HBM per device.

```python
import math
import jax
import jax.numpy as jnp
from jax import lax

PERMS = 64
SAMPLES = 65536
VARIANTS = 8192


def draw_genotypes(key, part):
    key_rate = jax.random.fold_in(key, 11)
    key_first = jax.random.fold_in(key, 12)
    key_second = jax.random.fold_in(key, 13)
    key_shared = jax.random.fold_in(key, 14)
    key_scale = jax.random.fold_in(key, 15)
    key_noise = jax.random.fold_in(key, 16)
    frequency = jax.random.randint(key_rate, (1, VARIANTS), 20, 500).astype(jnp.float32) / 1000.0
    first = jax.random.uniform(key_first, (SAMPLES, VARIANTS), jnp.float32) < frequency
    second = jax.random.uniform(key_second, (SAMPLES, VARIANTS), jnp.float32) < frequency
    position = (jnp.arange(SAMPLES, dtype=jnp.float32) / SAMPLES)[:, None]
    inbreeding = 0.6 * position
    low_scale, high_scale = (0.05, 0.4)
    shared = jax.random.uniform(key_shared, (SAMPLES, 1), jnp.float32) < inbreeding
    second = jnp.where(shared, first, second)
    hard = first.astype(jnp.float32) + second.astype(jnp.float32)
    scale = jnp.exp(jax.random.uniform(key_scale, (1, VARIANTS), jnp.float32, jnp.log(low_scale), jnp.log(high_scale)))
    noise = jax.random.uniform(key_noise, (SAMPLES, VARIANTS), jnp.float32, -1.0, 1.0) * scale
    return jnp.clip(hard + noise, 0.0, 2.0).astype(jnp.bfloat16)


def bell_draw(own_key, shape, scale, bound, kind=jnp.bfloat16):
    drawn = scale * jax.random.normal(own_key, shape, jnp.float32)
    return jnp.clip(drawn, min=-bound, max=bound).astype(kind)


def setup_inputs(seed: int = 0) -> dict:
    seeds = jax.random.split(jax.random.key(seed), 4)
    phenotype = bell_draw(seeds[0], (SAMPLES,), 1.0, 6.0, jnp.float32)
    perm_index = jax.vmap(lambda own: jax.random.permutation(own, SAMPLES))(jax.random.split(seeds[1], PERMS)).reshape((PERMS, SAMPLES)).astype(jnp.int32)
    genotypes = draw_genotypes(jax.random.fold_in(seeds[3], 71), 0)
    return {"phenotype": phenotype, "perm_index": perm_index, "genotypes": genotypes}


def reference(phenotype, perm_index, genotypes):
    centred = phenotype - jnp.mean(phenotype)
    sigma2 = jnp.mean(centred * centred) + 1e-05
    permuted = jnp.take(centred, perm_index, axis=0).astype(jnp.bfloat16)
    width = math.gcd(VARIANTS, 512)
    blocks = VARIANTS // width

    def one_block(index):
        start = (index * width).astype(jnp.int32)
        block = lax.dynamic_slice_in_dim(genotypes, start, width, 1)
        scores = jnp.dot(permuted, block, preferred_element_type=jnp.float32)
        wide = block.astype(jnp.float32)
        count = lax.optimization_barrier(jnp.sum(wide, axis=0))
        square = lax.optimization_barrier(jnp.sum(wide * wide, axis=0))
        spread = square - count * count / SAMPLES + 1.0
        return scores / jnp.sqrt(sigma2 * spread)[None, :]
    pieces = lax.map(one_block, jnp.arange(blocks, dtype=jnp.int32))
    statistics = jnp.transpose(pieces, (1, 0, 2)).reshape(PERMS, VARIANTS)
    largest = lax.optimization_barrier(jnp.max(jnp.abs(statistics), axis=1))
    return (statistics, largest)
```

```python
import functools

import jax
import jax.numpy as jnp
from jax import lax
from jax.experimental import pallas as pl
from jax.experimental.pallas import tpu as pltpu
from jax.sharding import PartitionSpec as P

MESH = pl.DeviceIdType.MESH
F32 = jnp.float32
BF16 = jnp.bfloat16
CHUNKS = 4
G_COPIES = 4


def kernel(dims, phen_hbm, idx_hbm, g_hbm, stat_out, max_out, phen, table, idx, g, perm, perm16, scores, from_core,
           chip_sum, from_y, y_sum, from_z, mom, mom_core, mom_y, mom_y_sum, mom_z, top, from_x, local_sem, ag_send,
           ag_recv, mom_send, mom_recv, core_send, core_recv, y_send, y_recv, z_send, z_recv, x_send, x_recv):
    ny, nz, nx = dims
    local = idx.shape[1]
    columns = g.shape[1]
    width = columns // CHUNKS
    lanes = columns // 128
    samples = phen.shape[0] * 128
    s = lax.axis_index("samp")
    v = lax.axis_index("var")
    core = lax.rem(s, 2)
    z = lax.rem(lax.div(s, 2), nz)
    y = lax.div(s, 2 * nz)

    def at(yy, zz, cc, vv):
        return ((yy * nz + zz) * 2 + cc, vv)

    def y_peer(d):
        return lax.rem(y + d, ny)

    def z_peer(d):
        return lax.rem(z + d, nz)

    def x_peer(d):
        return lax.rem(v + d, nx)

    partner = at(y, z, 1 - core, v)
    peers = [partner]
    peers += [at(y_peer(d), z, core, v) for d in range(1, ny)]
    peers += [at(y, z_peer(d), core, v) for d in range(1, nz)]
    peers += [at(y, z, core, x_peer(d)) for d in range(1, nx)]

    own_core = lax.div(v, nx // 2)
    own_y = lax.rem(v, nx // 2) * (2 * ny // nx)
    rows = idx.shape[0]

    phen_copy = pltpu.make_async_copy(phen_hbm, phen, local_sem.at[0])
    phen_copy.start()
    idx_copy = pltpu.make_async_copy(
        idx_hbm.at[pl.ds(pl.multiple_of(own_y * 2 * nz, 8), rows), :], idx, local_sem.at[1]
    )
    idx_copy.start()
    step = local // G_COPIES
    g_copies = [
        pltpu.make_async_copy(g_hbm.at[pl.ds(k * step, step), :], g.at[pl.ds(k * step, step), :], local_sem.at[2 + k])
        for k in range(G_COPIES)
    ]
    for copy in g_copies:
        copy.start()

    barrier = pltpu.get_barrier_semaphore()
    for peer in peers:
        pl.semaphore_signal(barrier, inc=1, device_id=peer, device_id_type=MESH)

    phen_copy.wait()
    trait = phen[...]
    mean = jnp.sum(trait, keepdims=True) / samples
    centred = trait - mean
    sigma2 = jnp.sum(centred * centred, keepdims=True) / samples + 1e-05
    half = phen.shape[0] // 2
    table[:, :128] = centred[:half].astype(BF16)
    table[:, 128:] = centred[half:].astype(BF16)
    idx_copy.wait()

    sent = []

    def send(src, dst, send_sem, recv_sem, peer):
        copy = pltpu.make_async_remote_copy(
            src_ref=src, dst_ref=dst, send_sem=send_sem, recv_sem=recv_sem, device_id=peer, device_id_type=MESH
        )
        copy.start()
        sent.append(copy)
        return copy

    places = lax.broadcasted_iota(jnp.int32, (256, 256), 0)
    own_rows = rows // 2
    base = v * own_rows
    ag = []
    for block in range(own_rows // 8):

        def look_up(k, carry):
            index = idx[pl.ds(2 * (block * 8 + k) + own_core, 1), :]
            inner = (index & 127) | ((index >> 15) << 7)
            outer = (index >> 7) & 255
            for start in range(0, local, 256):
                one_hot = jnp.where(places == inner[:, start : start + 256], 1.0, 0.0).astype(BF16)
                picked = jnp.dot(table[...], one_hot, preferred_element_type=F32)
                chosen = jnp.where(places == outer[:, start : start + 256], picked, 0.0)
                perm[pl.ds(base + block * 8 + k, 1), start : start + 256] = jnp.sum(chosen, axis=0, keepdims=True)
            return carry

        lax.fori_loop(0, 8, look_up, 0)
        if block == 0:
            pl.semaphore_wait(barrier, len(peers))
        part = perm.at[pl.ds(pl.multiple_of(base + block * 8, 8), 8), :]
        for d in range(1, nx):
            ag.append(
                send(part, part, ag_send.at[d - 1, block], ag_recv.at[d - 1, block], at(y, z, core, x_peer(d)))
            )

    for copy in g_copies:
        copy.wait()
    for block in range(columns // 256):

        def add_rows(i, sums):
            piece = g[pl.ds(pl.multiple_of(i * 64, 64), 64), block * 256 : (block + 1) * 256].astype(F32)
            piece = piece.reshape(8, 8, 256)
            return sums[0] + jnp.sum(piece, axis=0), sums[1] + jnp.sum(piece * piece, axis=0)

        zero = jnp.zeros((8, 256), F32)
        sums = lax.fori_loop(0, local // 64, add_rows, (zero, zero))
        for q in range(2):
            line = jnp.sum(sums[q], axis=0, keepdims=True)
            for j in range(2):
                mom[q, pl.ds(2 * block + j, 1), :] = line[:, j * 128 : (j + 1) * 128]

    mom_copy = send(mom, mom_core, mom_send.at[0], mom_recv.at[0], partner)
    for copy in ag:
        copy.wait_recv()
    perm16[...] = perm[...].astype(BF16)

    mine = core * (ny * nz)
    other = (1 - core) * (ny * nz)
    core_copies = []
    for c in range(CHUNKS):
        cols = pl.ds(c * width, width)
        scores[:, cols] = jnp.dot(perm16[...], g[:, cols], preferred_element_type=F32)
        core_copies.append(
            send(
                scores.at[pl.ds(pl.multiple_of(other, 8), ny * nz), cols],
                from_core.at[:, cols],
                core_send.at[c],
                core_recv.at[c],
                partner,
            )
        )

    mom_copy.wait_recv()
    mom_core[...] = mom[...] + mom_core[...]
    mom_copies = [
        send(mom_core, mom_y.at[d - 1], mom_send.at[d], mom_recv.at[d], at(y_peer(d), z, core, v))
        for d in range(1, ny)
    ]

    y_copies = []
    for c in range(CHUNKS):
        cols = pl.ds(c * width, width)
        core_copies[c].wait_recv()
        chip_sum[:, cols] = scores[pl.ds(pl.multiple_of(mine, 8), ny * nz), cols] + from_core[:, cols]
        y_copies.append([
            send(
                chip_sum.at[pl.ds(pl.multiple_of(y_peer(d) * nz, 8), nz), cols],
                from_y.at[d - 1, :, cols],
                y_send.at[d - 1, c],
                y_recv.at[d - 1, c],
                at(y_peer(d), z, core, v),
            )
            for d in range(1, ny)
        ])

    for copy in mom_copies:
        copy.wait_recv()
    total = mom_core[...]
    for d in range(1, ny):
        total = total + mom_y[d - 1]
    mom_y_sum[...] = total
    mom_copies = [
        send(mom_y_sum, mom_z.at[d - 1], mom_send.at[ny - 1 + d], mom_recv.at[ny - 1 + d], at(y, z_peer(d), core, v))
        for d in range(1, nz)
    ]

    z_copies = []
    for c in range(CHUNKS):
        cols = pl.ds(c * width, width)
        for copy in y_copies[c]:
            copy.wait_recv()
        total = chip_sum[pl.ds(pl.multiple_of(y * nz, 8), nz), cols]
        for d in range(1, ny):
            total = total + from_y[d - 1, :, cols]
        part_lanes = width // 128
        for j in range(part_lanes):
            for k in range(nz):
                y_sum[k, pl.ds(c * part_lanes + j, 1), :] = total[k : k + 1, j * 128 : (j + 1) * 128]
        lines = pl.ds(c * part_lanes, part_lanes)
        z_copies += [
            send(
                y_sum.at[z_peer(d), lines, :],
                from_z.at[d - 1, lines, :],
                z_send.at[d - 1, c],
                z_recv.at[d - 1, c],
                at(y, z_peer(d), core, v),
            )
            for d in range(1, nz)
        ]

    for copy in mom_copies:
        copy.wait_recv()
    moments = mom_y_sum[...]
    for d in range(1, nz):
        moments = moments + mom_z[d - 1]
    spread = moments[1] - moments[0] * moments[0] / samples + 1.0
    scale = jnp.sqrt(sigma2 * spread)
    for copy in z_copies:
        copy.wait_recv()
    total = y_sum[z]
    for d in range(1, nz):
        total = total + from_z[d - 1]
    statistic = total / scale
    stat_out[...] = statistic
    top[...] = jnp.broadcast_to(jnp.max(jnp.abs(statistic), keepdims=True), top.shape)
    x_copies = [
        send(top, from_x.at[d - 1], x_send.at[d - 1], x_recv.at[d - 1], at(y, z, core, x_peer(d)))
        for d in range(1, nx)
    ]
    for copy in x_copies:
        copy.wait_recv()
    largest = top[...]
    for d in range(1, nx):
        largest = jnp.maximum(largest, from_x[d - 1])
    max_out[...] = largest
    for copy in sent:
        copy.wait_send()


def solution(mesh):
    nx = mesh.shape["var"]
    ny, nz = 4, mesh.shape["samp"] // 8
    dims = (ny, nz, nx)

    def on_device(phenotype, perm_index, genotypes):
        perms, local = perm_index.shape
        columns = genotypes.shape[1]
        lanes = columns // 128
        samples = phenotype.shape[0]
        own = perms // nx
        anywhere = pl.BlockSpec(memory_space=pl.ANY)
        vmem = pl.BlockSpec(memory_space=pltpu.VMEM)
        dma = pltpu.SemaphoreType.DMA
        statistics, largest = pl.pallas_call(
            functools.partial(kernel, dims),
            out_shape=(
                jax.ShapeDtypeStruct((lanes, 128), F32),
                jax.ShapeDtypeStruct((1, 128), F32),
            ),
            in_specs=[anywhere] * 3,
            out_specs=(vmem, vmem),
            scratch_shapes=[
                pltpu.VMEM((samples // 128, 128), F32),
                pltpu.VMEM((256, 256), BF16),
                pltpu.VMEM((2 * own, local), jnp.int32),
                pltpu.VMEM((local, columns), BF16),
                pltpu.VMEM((perms, local), F32),
                pltpu.VMEM((perms, local), BF16),
                pltpu.VMEM((perms, columns), F32),
                pltpu.VMEM((perms // 2, columns), F32),
                pltpu.VMEM((perms // 2, columns), F32),
                pltpu.VMEM((ny - 1, nz, columns), F32),
                pltpu.VMEM((nz, lanes, 128), F32),
                pltpu.VMEM((nz - 1, lanes, 128), F32),
                pltpu.VMEM((2, lanes, 128), F32),
                pltpu.VMEM((2, lanes, 128), F32),
                pltpu.VMEM((ny - 1, 2, lanes, 128), F32),
                pltpu.VMEM((2, lanes, 128), F32),
                pltpu.VMEM((nz - 1, 2, lanes, 128), F32),
                pltpu.VMEM((1, 128), F32),
                pltpu.VMEM((nx - 1, 1, 128), F32),
                dma((2 + G_COPIES,)),
                dma((nx - 1, own // 8)),
                dma((nx - 1, own // 8)),
                dma((ny + nz - 1,)),
                dma((ny + nz - 1,)),
                dma((CHUNKS,)),
                dma((CHUNKS,)),
                dma((ny - 1, CHUNKS)),
                dma((ny - 1, CHUNKS)),
                dma((nz - 1, CHUNKS)),
                dma((nz - 1, CHUNKS)),
                dma((nx - 1,)),
                dma((nx - 1,)),
            ],
            compiler_params=pltpu.CompilerParams(
                collective_id=0, has_side_effects=True, vmem_limit_bytes=40 * 1024 * 1024
            ),
        )(phenotype.reshape(samples // 128, 128), perm_index, genotypes)
        return statistics.reshape(1, columns), largest[0, :1]

    return jax.shard_map(
        on_device,
        mesh=mesh,
        in_specs=(P(), P(None, "samp"), P("samp", "var")),
        out_specs=(P("samp", "var"), P("samp")),
        check_vma=False,
    )
```
